32 devices in a mesh: member: 2 (over x), dp: 8 (over z, y), mp: 2 (over core).
Axes of the slice: x: 2, y: 2, z: 4, core: 2. Of those that a mesh axis runs over, the one named last changes fastest.
Arguments:
- activations: bfloat16 [2048, 2048], P(('member', 'dp')), parts along dimension 0, may hold values from -6 to 6
- out_grads: bfloat16 [2048, 10240], P(('member', 'dp'), 'mp'), parts along dimension 0, may hold values from -0.19921875 to 0.19921875
- slot_table: int32 [4, 16], P(('member', 'mp')), parts along dimension 0, may hold values from 0 to 15, each once within a row
- exponent_index: int32 [4, 16], P(('member', 'mp')), parts along dimension 0, may hold values from 0 to 1
- damping_index: int32 [4, 16], P(('member', 'mp')), parts along dimension 0, may hold values from 0 to 3
Outputs:
- update: bfloat16 [4096, 10240], P('member', 'mp'), parts along dimension 0
- preconditioners: bfloat16 [4, 16, 2, 1024, 1024], P(('member', 'mp'), 'dp'), parts along dimension 0
The draws below stay inside these ranges and needn't reach their ends.
There are 2 independent parts, one for each index of `member`. The reference program is written for one: setup_inputs(seed, part) draws one part's arguments, and reference() takes and returns one part's arrays. A program takes and returns all parts, laid end to end along the dimension named above; each array names one. Nothing has to cross between parts.
Inputs may be any that keep to these rules, and one draw needn't show every extreme that they name: `slot_table`: each row is a permutation of 0 to 15; slot s belongs to dp index s.
All inputs are finite; a program needn't handle non-finite values.
Results may differ from the reference program's by a relative error of at most 0.006.
The reference program's roundings to bfloat16 on the way (of `gradient`, `half_step` and `assembled`) count: a program that leaves them out, or rounds other values in their place, can miss the bound.
Values may be sent and summed in bfloat16 or wider, within the bound.
No kernel may reach another device: no remote copies, remote signals or barrier semaphores. Data moves between devices by JAX's collectives and lax.ppermute only.
A program may use at most 192 MiB of HBM per device.

```python
import jax
import jax.numpy as jnp
from jax import lax

D_WIN = 2048
FF_WIN = 10240
BLK = 1024
SLOTS = 16
ITERS = 2
TOKENS = 1024
N_MP = 2


def plant(entries, stream_key, least, top_value):
    index_at = [jax.random.randint(jax.random.fold_in(stream_key, axis), (), 0, length) for axis, length in enumerate(entries.shape)]
    widest = entries.shape.index(max(entries.shape))
    neighbour = index_at[:widest] + [(index_at[widest] + 1) % entries.shape[widest]] + index_at[widest + 1:]
    return entries.at[tuple(index_at)].set(least).at[tuple(neighbour)].set(top_value)


def block_levels(own_key, dims, cuts, low, top_value):
    factor_of, own = 1.0, jax.random.fold_in(own_key, 6)
    for dim, shards_of in cuts:
        heights = jnp.exp(jax.random.uniform(jax.random.fold_in(own, dim), (shards_of,), jnp.float32, low / len(cuts), top_value / len(cuts)))
        factor_of = factor_of * jnp.repeat(heights, dims[dim] // shards_of).reshape([-1 if axis == dim else 1 for axis in range(len(dims))])
    return factor_of


def gaussian(key, extent, width, bound, split=(), kind=jnp.bfloat16):
    array = width * jax.random.normal(key, extent, jnp.float32)
    if split:
        array = array * block_levels(key, extent, split, -0.22, 0.18)
    return jnp.clip(array, -bound, bound).astype(kind)


def setup_inputs(seed: int = 0, part: int = 0) -> dict:
    keys = jax.random.split(jax.random.key(seed), 6)
    part_keys = jax.random.split(jax.random.fold_in(keys[5], part), 6)
    activations = gaussian(part_keys[0], (TOKENS, D_WIN), 1.0, 6.0, ((0, 8),))
    out_grads = gaussian(part_keys[1], (TOKENS, FF_WIN), 0.03125, 0.19921875, ((0, 8), (1, 2)))
    slot_table = jax.vmap(lambda own: jax.random.permutation(own, SLOTS))(jax.random.split(part_keys[2], N_MP)).reshape((N_MP, SLOTS)).astype(jnp.int32)
    exponent_index = plant(jax.random.randint(part_keys[3], (N_MP, SLOTS), 0, 2), jax.random.fold_in(part_keys[3], 1), 0, 1).astype(jnp.int32)
    damping_index = plant(jax.random.randint(part_keys[4], (N_MP, SLOTS), 0, 4), jax.random.fold_in(part_keys[4], 1), 0, 3).astype(jnp.int32)
    return dict(activations=activations, out_grads=out_grads, slot_table=slot_table, exponent_index=exponent_index, damping_index=damping_index)


ROOT_ORDERS = (2.0, 4.0)
DAMPINGS = (0.03, 0.1, 0.3, 1.0)

def table_value(picked, values_table):
    values = jnp.asarray(values_table, jnp.float32)
    matches = jnp.arange(len(values_table), dtype=jnp.int32) == picked
    return jnp.sum(jnp.where(matches, values, 0.0))

def half_dot(first, second):
    return jnp.dot(first.astype(jnp.bfloat16), second.astype(jnp.bfloat16), preferred_element_type=jnp.float32)

def inverse_root(statistic, root_order, quartic, damping):
    dimension = statistic.shape[0]
    identity = jnp.eye(dimension, dtype=jnp.float32)
    damped = statistic + damping * (jnp.trace(statistic) / dimension + 1.0) * identity
    current = damped * (dimension / (2.0 * jnp.trace(damped)))
    factor = ((root_order + 1.0) * identity - current) / root_order
    estimate = factor
    for sweep in range(1, ITERS):
        square = half_dot(factor, factor)
        fourth = half_dot(square, square)
        raised = jnp.where(quartic, fourth, square)
        current = half_dot(raised, current)
        factor = ((root_order + 1.0) * identity - current) / root_order
        estimate = half_dot(estimate, factor)
    return estimate.astype(jnp.bfloat16)

def precondition(act_block, grad_block, root_order, quartic, damping):
    gradient = lax.dot_general(act_block, grad_block, (((0,), (0,)), ((), ())), preferred_element_type=jnp.float32).astype(jnp.bfloat16)
    left_stat = lax.dot_general(gradient, gradient, (((1,), (1,)), ((), ())), preferred_element_type=jnp.float32)
    right_stat = lax.dot_general(gradient, gradient, (((0,), (0,)), ((), ())), preferred_element_type=jnp.float32)
    left_root = inverse_root(left_stat, root_order, quartic, damping)
    right_root = inverse_root(right_stat, root_order, quartic, damping)
    half_step = jnp.dot(left_root, gradient, preferred_element_type=jnp.float32).astype(jnp.bfloat16)
    block_update = jnp.dot(half_step, right_root, preferred_element_type=jnp.float32).astype(jnp.bfloat16)
    return (block_update, jnp.stack([left_root, right_root]))

def reference(activations, out_grads, slot_table, exponent_index, damping_index):
    row_blocks = D_WIN // BLK
    col_blocks = FF_WIN // (N_MP * BLK)
    half_blocks = row_blocks * col_blocks
    acts_grid = activations.reshape(TOKENS, row_blocks, BLK)
    grads_grid = out_grads.reshape(TOKENS, N_MP, col_blocks, BLK)
    flat_exp = exponent_index.reshape(N_MP * SLOTS)
    flat_damp = damping_index.reshape(N_MP * SLOTS)

    def one_slot(flat_slot):
        half_id = flat_slot // SLOTS
        slot_id = flat_slot % SLOTS
        exp_pick = lax.dynamic_index_in_dim(flat_exp, flat_slot, 0, keepdims=False)
        damp_pick = lax.dynamic_index_in_dim(flat_damp, flat_slot, 0, keepdims=False)
        root_order = table_value(exp_pick, ROOT_ORDERS)
        quartic = exp_pick == 1
        damping = table_value(damp_pick, DAMPINGS)
        table_row = lax.dynamic_index_in_dim(slot_table, half_id, 0, keepdims=False)[:half_blocks]
        matches = table_row == slot_id
        filled = jnp.any(matches)
        block_id = jnp.sum(jnp.where(matches, jnp.arange(half_blocks, dtype=jnp.int32), 0)).astype(jnp.int32)
        act_block = lax.dynamic_index_in_dim(acts_grid, block_id // col_blocks, 1, keepdims=False)
        grad_half = lax.dynamic_index_in_dim(grads_grid, half_id, 1, keepdims=False)
        grad_block = lax.dynamic_index_in_dim(grad_half, block_id % col_blocks, 1, keepdims=False)
        act_block = jnp.where(filled, act_block, jnp.zeros_like(act_block))
        grad_block = jnp.where(filled, grad_block, jnp.zeros_like(grad_block))
        return precondition(act_block, grad_block, root_order, quartic, damping)
    block_updates, roots = lax.map(one_slot, jnp.arange(N_MP * SLOTS, dtype=jnp.int32))
    by_slot = block_updates.reshape(N_MP, SLOTS, BLK, BLK)
    chosen = jnp.take_along_axis(by_slot, slot_table[:, :half_blocks][:, :, None, None], axis=1)
    assembled = chosen.reshape(N_MP, row_blocks, col_blocks, BLK, BLK).transpose(1, 3, 0, 2, 4).reshape(D_WIN, FF_WIN)
    wide = assembled.astype(jnp.float32)
    total_sq = jnp.sum(wide * wide)
    rescale = lax.rsqrt(total_sq / (D_WIN * FF_WIN) + 1.0)
    update = (wide * rescale).astype(jnp.bfloat16)
    return (update, roots.reshape(N_MP, SLOTS, 2, BLK, BLK))
```

```python
import jax
import jax.numpy as jnp
from jax import lax
from jax.sharding import PartitionSpec as P

BLK = 1024
ROOT_ORDERS = (2.0, 4.0)
DAMPINGS = (0.03, 0.1, 0.3, 1.0)


def table_value(picked, values_table):
    values = jnp.asarray(values_table, jnp.float32)
    matches = jnp.arange(len(values_table), dtype=jnp.int32) == picked
    return jnp.sum(jnp.where(matches, values, 0.0))


def bf16_dot(first, second, contract):
    return lax.dot_general(
        first, second, ((contract[:1], contract[1:]), ((), ())), preferred_element_type=jnp.float32
    )


def block_gradient(act_block, grad_block):
    return bf16_dot(act_block, grad_block, (0, 0)).astype(jnp.bfloat16)


def inverse_root(gradient, axis, square_sum, params):
    root_order, quartic, damping = params
    side = gradient.shape[0]
    eye = jnp.eye(side, dtype=jnp.float32)
    shift = damping * (square_sum / side + 1.0)
    scale = side / (2.0 * (square_sum + side * shift))
    statistic = bf16_dot(gradient, gradient, (axis, axis))
    current = (statistic + shift * eye) * scale
    factor = (((root_order + 1.0) * eye - current) / root_order).astype(jnp.bfloat16)
    current = current.astype(jnp.bfloat16)
    square = bf16_dot(factor, factor, (1, 0)).astype(jnp.bfloat16)
    fourth = bf16_dot(square, square, (1, 0)).astype(jnp.bfloat16)
    raised = jnp.where(quartic, fourth, square)
    later = bf16_dot(raised, current, (1, 0))
    later = (((root_order + 1.0) * eye - later) / root_order).astype(jnp.bfloat16)
    return bf16_dot(factor, later, (1, 0)).astype(jnp.bfloat16)


def block_roots(gradient, params):
    wide = gradient.astype(jnp.float32)
    square_sum = jnp.sum(wide * wide)
    left_root = inverse_root(gradient, 1, square_sum, params)
    right_root = inverse_root(gradient, 0, square_sum, params)
    return left_root, right_root


def block_update(gradient, params):
    left_root, right_root = block_roots(gradient, params)
    half_step = bf16_dot(left_root, gradient, (1, 0)).astype(jnp.bfloat16)
    update = bf16_dot(half_step, right_root, (1, 0)).astype(jnp.bfloat16)
    wide = update.astype(jnp.float32)
    return update, jnp.sum(wide * wide)


def ring_pairs(count):
    order = list(range(0, count, 2)) + list(range(1, count, 2))[::-1]
    ahead = [(order[i], order[(i + 1) % count]) for i in range(count)]
    back = [(b, a) for a, b in ahead]
    return order, ahead, back


def on_device(activations, out_grads, slot_table, exponent_index, damping_index):
    tok_count = activations.shape[0]
    row_blocks = activations.shape[1] // BLK
    half_width = out_grads.shape[1]
    col_blocks = half_width // BLK
    half_blocks = row_blocks * col_blocks
    owners = lax.axis_size("dp")
    halves = lax.axis_size("mp")
    me = lax.axis_index("dp")
    core = lax.axis_index("mp")
    slot_count = slot_table.shape[1]
    per_owner = slot_count // owners
    order, ahead, back = ring_pairs(owners)
    order_of = jnp.asarray(order, jnp.int32)
    place_of = jnp.asarray([order.index(i) for i in range(owners)], jnp.int32)
    place = place_of[me]

    def source_of(step):
        return order_of[(place + step) % owners]

    part = activations.shape[1] // halves
    act_part = lax.dynamic_slice(activations, (0, core * part), (tok_count, part))
    half_tok = tok_count // 2
    grads_all = jnp.zeros((owners * tok_count, half_width), jnp.bfloat16)
    acts_all = jnp.zeros((owners * tok_count, activations.shape[1]), jnp.bfloat16)
    mp_shifts = [[(i, (i + s) % halves) for i in range(halves)] for s in range(1, halves)]

    def keep(grads_all, acts_all, source, lower, grads, acts):
        row = source * tok_count + lower * half_tok
        grads_all = lax.dynamic_update_slice(grads_all, grads, (row, 0))
        acts_all = lax.dynamic_update_slice(acts_all, acts, (row, 0))
        for turn, shift in enumerate(mp_shifts):
            other = lax.ppermute(acts, "mp", shift)
            acts_all = lax.dynamic_update_slice(acts_all, other, (row, (turn + 1) * part))
        return grads_all, acts_all

    down = (out_grads[:half_tok], act_part[:half_tok])
    up = (out_grads[half_tok:], act_part[half_tok:])
    for step in range(owners):
        if step:
            down = tuple(lax.ppermute(piece, "dp", ahead) for piece in down)
            up = tuple(lax.ppermute(piece, "dp", back) for piece in up)
        grads_all, acts_all = keep(grads_all, acts_all, source_of(-step), 0, *down)
        grads_all, acts_all = keep(grads_all, acts_all, source_of(step), 1, *up)

    table = slot_table[0, :half_blocks]
    exponents = exponent_index[0]
    dampings = damping_index[0]

    def slot_params(slot):
        exp_pick = exponents[slot]
        return (
            table_value(exp_pick, ROOT_ORDERS),
            exp_pick == 1,
            table_value(dampings[slot], DAMPINGS),
        )

    def gradient_of(block):
        row_at = (block // col_blocks) * BLK
        col_at = (block % col_blocks) * BLK
        behind = (row_at + (halves - core) * part) % (halves * part)
        turn_at = ((halves - behind // part) % halves) * part + behind % part
        act_block = lax.dynamic_slice(acts_all, (0, turn_at), (owners * tok_count, BLK))
        grad_block = lax.dynamic_slice(grads_all, (0, col_at), (owners * tok_count, BLK))
        return block_gradient(act_block, grad_block)

    shared = min(owners, half_blocks)
    mine = jnp.minimum(me, shared - 1)
    update_piece, piece_sq = block_update(gradient_of(mine), slot_params(table[mine]))
    piece_sq = jnp.where(me < shared, piece_sq, 0.0)

    rest = []
    rest_sq = 0.0
    for block in range(shared, half_blocks):
        update, update_sq = block_update(gradient_of(block), slot_params(table[block]))
        rest.append((block, update))
        rest_sq = rest_sq + update_sq

    roots = []
    for position in range(per_owner):
        slot = me * per_owner + position
        matches = table == slot
        filled = jnp.any(matches)
        block = jnp.sum(jnp.where(matches, jnp.arange(half_blocks, dtype=jnp.int32), 0))
        gradient = gradient_of(block)
        gradient = jnp.where(filled, gradient, jnp.zeros_like(gradient))
        roots.append(jnp.stack(block_roots(gradient, slot_params(slot))))

    bit = 1
    while bit < owners:
        pairs = [(i, i ^ bit) for i in range(owners)]
        piece_sq = piece_sq + lax.ppermute(piece_sq, "dp", pairs)
        bit *= 2
    half_sq = piece_sq + rest_sq
    bit = 1
    while bit < halves:
        pairs = [(i, i ^ bit) for i in range(halves)]
        half_sq = half_sq + lax.ppermute(half_sq, "mp", pairs)
        bit *= 2
    rescale = lax.rsqrt(half_sq / (row_blocks * BLK * half_width * halves) + 1.0)

    canvas = jnp.zeros((row_blocks * BLK, half_width), jnp.bfloat16)

    def put(canvas, block, lower, piece):
        row_at = (block // col_blocks) * BLK + lower
        col_at = (block % col_blocks) * BLK
        scaled = (piece.astype(jnp.float32) * rescale).astype(jnp.bfloat16)
        return lax.dynamic_update_slice(canvas, scaled, (row_at, col_at))

    for block, update in rest:
        canvas = put(canvas, block, 0, update)
    rows = BLK // 2
    down, up = update_piece[:rows], update_piece[rows:]
    for step in range(owners):
        if step:
            down = lax.ppermute(down, "dp", ahead)
            up = lax.ppermute(up, "dp", back)
        canvas = put(canvas, jnp.minimum(source_of(-step), shared - 1), 0, down)
        canvas = put(canvas, jnp.minimum(source_of(step), shared - 1), rows, up)
    return canvas, jnp.stack(roots)[None]


def solution(mesh):
    placed = (
        P(("member", "dp"), None),
        P(("member", "dp"), "mp"),
        P(("member", "mp"), None),
        P(("member", "mp"), None),
        P(("member", "mp"), None),
    )
    return jax.shard_map(
        on_device,
        mesh=mesh,
        in_specs=placed,
        out_specs=(P("member", "mp"), P(("member", "mp"), "dp", None, None, None)),
        check_vma=False,
    )
```

```python
import functools

import jax
import jax.numpy as jnp
from jax import lax
from jax.experimental import pallas as pl
from jax.experimental.pallas import tpu as pltpu
from jax.sharding import PartitionSpec as P

BLK = 1024
ROOT_ORDERS = (2.0, 4.0)
DAMPINGS = (0.03, 0.1, 0.3, 1.0)
HBM = pltpu.MemorySpace.HBM
VMEM_LIMIT = 60 * 2**20


def table_value(picked, values_table):
    values = jnp.asarray(values_table, jnp.float32)
    matches = jnp.arange(len(values_table), dtype=jnp.int32) == picked[:, None]
    return jnp.sum(jnp.where(matches, values, 0.0), axis=1)


def wide_dot(first, second, first_dim, second_dim):
    return lax.dot_general(
        first, second, (((first_dim,), (second_dim,)), ((), ())), preferred_element_type=jnp.float32
    )


def gather_block(ints, places, sources, acts_t, grads, sems):
    owners, turns, tok, grad_refs, act_refs = sources
    turn, column = ints[0], ints[1]
    columns = pl.ds(pl.multiple_of(column * BLK, BLK), BLK)
    half_tok = tok // 2
    half_row = BLK // 2
    waits = []

    def start(copy_of, count):
        sem = sems.at[len(waits)]
        for index in range(count):
            if count == 1:
                copy_of(index, sem).start()
            else:
                pl.when(turn == index)(lambda index=index: copy_of(index, sem).start())
        waits.append(copy_of(0, sem))

    for step in range(owners):
        for way in range(2):
            if step == 0 and way == 1:
                continue
            source = places[way * owners + step]
            rows = tok if step == 0 else half_tok
            at_tok = pl.multiple_of(source * tok + (half_tok * way), half_tok)
            at_lane = pl.multiple_of(source * tok, tok)
            grad_ref = grad_refs[step * 2 + way]
            start(
                lambda _, sem, grad_ref=grad_ref, at_tok=at_tok, rows=rows: pltpu.make_async_copy(
                    grad_ref.at[:, columns], grads.at[pl.ds(at_tok, rows), :], sem
                ),
                1,
            )
            act_rows = slice(0, BLK) if step == 0 else slice(half_row * way, half_row * (way + 1))
            start(
                lambda index, sem, at_lane=at_lane, act_rows=act_rows, at=step * 2 + way: (
                    pltpu.make_async_copy(
                        act_refs[index][at], acts_t.at[act_rows, pl.ds(at_lane, tok)], sem
                    )
                ),
                turns,
            )
    for copy in waits:
        copy.wait()


def inverse_root(side, gradient, root, square_sum, params, current, factor, raised, later):
    root_order, quartic, damping = params
    shift = damping * (square_sum / BLK + 1.0)
    scale = BLK / (2.0 * (square_sum + BLK * shift))
    inverse = 1.0 / root_order
    eye = lax.broadcasted_iota(jnp.int32, (BLK, BLK), 0) == lax.broadcasted_iota(
        jnp.int32, (BLK, BLK), 1
    )
    statistic = wide_dot(gradient[side], gradient[side], 1, 1)
    scaled = jnp.where(eye, statistic + shift, statistic) * scale
    current[...] = scaled.astype(jnp.bfloat16)
    factor[...] = ((jnp.where(eye, root_order + 1.0, 0.0) - scaled) * inverse).astype(jnp.bfloat16)
    raised[0] = wide_dot(factor[...], factor[...], 1, 0).astype(jnp.bfloat16)

    @pl.when(quartic != 0)
    def _():
        raised[1] = wide_dot(raised[0], raised[0], 1, 0).astype(jnp.bfloat16)

    moved = wide_dot(raised[quartic], current[...], 1, 0)
    later[...] = ((jnp.where(eye, root_order + 1.0, 0.0) - moved) * inverse).astype(jnp.bfloat16)
    root[...] = wide_dot(factor[...], later[...], 1, 0).astype(jnp.bfloat16)


def block_kernel(kind, owners, turns, extra, job, position, *refs):
    refs = list(refs)
    int_table, float_table, places = refs[:3]
    ints = [int_table[4 * job + field] for field in range(4)]
    floats = [float_table[2 * job + field] for field in range(2)]
    chunks = 2 * owners - 1
    at = 3
    own = refs[at : at + chunks]
    grad_refs = [own[0], None] + own[1:]
    at += chunks
    act_refs = []
    for _ in range(turns):
        own = refs[at : at + chunks]
        act_refs.append([own[0], None] + own[1:])
        at += chunks
    tok = grad_refs[0].shape[0]
    left_in = None
    if kind == "finish":
        left_in = refs[at]
        at += 1
    at += extra
    outs = refs[at : at + (1 if kind in ("left", "roots") else 3)]
    at += len(outs)
    acts_t, grads, gradient, current, factor, raised, later, pair, sems, out_sems = refs[at:]
    gather_block(
        ints, places, (owners, turns, tok, grad_refs, act_refs), acts_t, grads, sems
    )
    block_grad = wide_dot(acts_t[...], grads[...], 1, 0)
    block_grad = jnp.where(ints[3] != 0, block_grad, 0.0).astype(jnp.bfloat16)
    gradient[0] = block_grad
    if kind != "left":
        gradient[1] = block_grad.T
    squares = block_grad.astype(jnp.float32)
    square_sum = jnp.sum(squares * squares)
    params = (floats[0], ints[2], floats[1])
    work = (current, factor, raised, later)
    if kind == "left":
        inverse_root(0, gradient, outs[0], square_sum, params, *work)
        return
    if kind == "finish":
        inverse_root(1, gradient, pair.at[1], square_sum, params, *work)
        left_root = left_in[...]
    else:

        def one_side(side, carry):
            inverse_root(side, gradient, pair.at[side], square_sum, params, *work)
            if kind == "roots":
                pltpu.make_async_copy(
                    pair.at[side], outs[0].at[position, side], out_sems.at[side]
                ).start()
            return carry

        lax.fori_loop(0, 2, one_side, 0)
        left_root = pair[0]
    if kind == "roots":
        for side in range(2):
            pltpu.make_async_copy(
                pair.at[side], outs[0].at[position, side], out_sems.at[side]
            ).wait()
        return
    later[...] = wide_dot(left_root, gradient[0], 1, 0).astype(jnp.bfloat16)
    update = wide_dot(later[...], pair[1], 1, 0).astype(jnp.bfloat16)
    outs[0][...] = update[: BLK // 2]
    outs[1][...] = update[BLK // 2 :]
    wide = update.astype(jnp.float32)
    outs[2][0, 0] = jnp.sum(wide * wide)


def run_block(kind, job, meta, chunks, left_root=None, roots=None, position=0, count=1, after=()):
    ints, floats, places = meta
    grad_chunks, act_chunks = chunks
    owners = (len(grad_chunks) + 1) // 2
    turns = len(act_chunks)
    tokens = owners * grad_chunks[0].shape[0]
    smem = pl.BlockSpec(memory_space=pltpu.SMEM)
    vmem = pl.BlockSpec(memory_space=pltpu.VMEM)
    hbm = pl.BlockSpec(memory_space=HBM)
    operands = [ints, floats, places, *grad_chunks]
    for turn in act_chunks:
        operands += turn
    specs = [smem] * 3 + [hbm] * (len(operands) - 3)
    if left_root is not None:
        operands.append(left_root)
        specs.append(vmem)
    aliases = {}
    if roots is not None:
        aliases = {len(operands): 0}
        after = (roots, *after)
    operands += after
    specs += [hbm] * len(after)
    half = jnp.bfloat16
    piece = jax.ShapeDtypeStruct((BLK // 2, BLK), half)
    if kind == "left":
        out_shape, out_specs = jax.ShapeDtypeStruct((BLK, BLK), half), vmem
    elif kind == "roots":
        out_shape, out_specs = jax.ShapeDtypeStruct((count, 2, BLK, BLK), half), hbm
    else:
        out_shape = (piece, piece, jax.ShapeDtypeStruct((1, 1), jnp.float32))
        out_specs = (vmem, vmem, smem)
    matmuls = {"left": 6, "roots": 11, "finish": 8, "both": 13}[kind]
    return pl.pallas_call(
        functools.partial(block_kernel, kind, owners, turns, len(after), job, position),
        out_shape=out_shape,
        in_specs=specs,
        out_specs=out_specs,
        input_output_aliases=aliases,
        scratch_shapes=[
            pltpu.VMEM((BLK, tokens), half),
            pltpu.VMEM((tokens, BLK), half),
            pltpu.VMEM((2, BLK, BLK), half),
            pltpu.VMEM((BLK, BLK), half),
            pltpu.VMEM((BLK, BLK), half),
            pltpu.VMEM((2, BLK, BLK), half),
            pltpu.VMEM((BLK, BLK), half),
            pltpu.VMEM((2, BLK, BLK), half),
            pltpu.SemaphoreType.DMA((2 * (2 * owners - 1),)),
            pltpu.SemaphoreType.DMA((2,)),
        ],
        compiler_params=pltpu.CompilerParams(vmem_limit_bytes=VMEM_LIMIT),
        cost_estimate=pl.CostEstimate(
            flops=matmuls * 2 * BLK**3, bytes_accessed=6 * 2 * BLK**2, transcendentals=0
        ),
        name="block_" + kind,
    )(*operands)


def place_kernel(count, extra, *refs):
    spots, rescale = refs[:2]
    pieces = refs[2 : 2 + count]
    canvas, held, in_sems, out_sems = refs[2 + count + extra :]
    rows = held.shape[1]
    loads = []
    stores = []
    for index in range(count):
        row = pl.multiple_of(spots[2 * index], rows)
        column = pl.multiple_of(spots[2 * index + 1], BLK)
        loads.append(pltpu.make_async_copy(pieces[index], held.at[index], in_sems.at[index]))
        stores.append(
            pltpu.make_async_copy(
                held.at[index],
                canvas.at[pl.ds(row, rows), pl.ds(column, BLK)],
                out_sems.at[index],
            )
        )
    for load in loads:
        load.start()
    for index in range(count):
        loads[index].wait()
        wide = held[index].astype(jnp.float32) * rescale[0, 0]
        held[index] = wide.astype(jnp.bfloat16)
        stores[index].start()
    for store in stores:
        store.wait()


def place_pieces(canvas, shape, spots, rescale, pieces):
    count = len(pieces)
    smem = pl.BlockSpec(memory_space=pltpu.SMEM)
    hbm = pl.BlockSpec(memory_space=HBM)
    old = [] if canvas is None else [canvas]
    return pl.pallas_call(
        functools.partial(place_kernel, count, len(old)),
        out_shape=jax.ShapeDtypeStruct(shape, jnp.bfloat16),
        in_specs=[smem, smem] + [hbm] * (count + len(old)),
        out_specs=hbm,
        input_output_aliases={2 + count: 0} if old else {},
        scratch_shapes=[
            pltpu.VMEM((count, *pieces[0].shape), jnp.bfloat16),
            pltpu.SemaphoreType.DMA((count,)),
            pltpu.SemaphoreType.DMA((count,)),
        ],
        compiler_params=pltpu.CompilerParams(vmem_limit_bytes=VMEM_LIMIT),
        cost_estimate=pl.CostEstimate(
            flops=count * BLK * BLK * 100, bytes_accessed=2 * count * BLK * BLK, transcendentals=0
        ),
        name="place",
    )(jnp.stack(spots).astype(jnp.int32), rescale, *pieces, *old)


def ring_pairs(count):
    order = list(range(0, count, 2)) + list(range(1, count, 2))[::-1]
    ahead = [(order[i], order[(i + 1) % count]) for i in range(count)]
    back = [(b, a) for a, b in ahead]
    return order, ahead, back


def on_device(activations, out_grads, slot_table, exponent_index, damping_index):
    tok_count = activations.shape[0]
    row_blocks = activations.shape[1] // BLK
    half_width = out_grads.shape[1]
    col_blocks = half_width // BLK
    half_blocks = row_blocks * col_blocks
    owners = lax.axis_size("dp")
    halves = lax.axis_size("mp")
    me = lax.axis_index("dp")
    core = lax.axis_index("mp")
    slot_count = slot_table.shape[1]
    per_owner = slot_count // owners
    order, ahead, back = ring_pairs(owners)
    order_of = jnp.asarray(order, jnp.int32)
    place = jnp.asarray([order.index(i) for i in range(owners)], jnp.int32)[me]
    steps = jnp.arange(owners, dtype=jnp.int32)
    from_behind = order_of[(place - steps) % owners]
    from_ahead = order_of[(place + steps) % owners]
    places = jnp.concatenate([from_behind, from_ahead])

    table = slot_table[0, :half_blocks]
    exponents = exponent_index[0]
    dampings = damping_index[0]

    shared = min(owners, half_blocks)
    mine = jnp.minimum(me, shared - 1)
    block_range = jnp.arange(half_blocks, dtype=jnp.int32)
    slot_range = jnp.arange(slot_count, dtype=jnp.int32)
    spread = jnp.concatenate([mine[None], block_range[shared:]])
    spread_slots = jnp.sum(
        jnp.where(spread[:, None] == block_range[None, :], table[None, :], 0), axis=1
    )
    own_slots = me * per_owner + jnp.arange(per_owner, dtype=jnp.int32)
    matches = own_slots[:, None] == table[None, :]
    own_blocks = jnp.sum(jnp.where(matches, block_range[None, :], 0), axis=1)
    blocks = jnp.concatenate([spread, own_blocks])
    slots = jnp.concatenate([spread_slots, own_slots])
    filled = jnp.concatenate([jnp.ones_like(spread), jnp.any(matches, axis=1).astype(jnp.int32)])
    at_slot = slots[:, None] == slot_range[None, :]
    exp_picks = jnp.sum(jnp.where(at_slot, exponents[None, :], 0), axis=1)
    damp_picks = jnp.sum(jnp.where(at_slot, dampings[None, :], 0), axis=1)
    turn = (core - blocks // col_blocks) % halves
    ints = jnp.stack([turn, blocks % col_blocks, exp_picks, filled], axis=1).reshape(-1)
    floats = jnp.stack(
        [table_value(exp_picks, ROOT_ORDERS), table_value(damp_picks, DAMPINGS)], axis=1
    ).reshape(-1)
    meta = (ints.astype(jnp.int32), floats, places)

    part = activations.shape[1] // halves
    assert part == BLK
    act_part = lax.dynamic_slice(activations, (0, core * part), (tok_count, part)).T
    mp_shifts = [[(i, (i + s) % halves) for i in range(halves)] for s in range(1, halves)]
    half_tok = tok_count // 2
    half_row = part // 2

    grad_chunks = [out_grads]
    act_chunks = [[act_part]]
    for shift in mp_shifts:
        act_chunks.append([lax.ppermute(act_part, "mp", shift)])
    down = (out_grads[:half_tok], act_part[:half_row])
    up = (out_grads[half_tok:], act_part[half_row:])
    for step in range(1, owners):
        down = tuple(lax.ppermute(piece, "dp", ahead) for piece in down)
        up = tuple(lax.ppermute(piece, "dp", back) for piece in up)
        if step == 2:
            down, up, meta = lax.optimization_barrier((down, up, meta))
        else:
            down, up = lax.optimization_barrier((down, up))
        grad_chunks += [down[0], up[0]]
        act_chunks[0] += [down[1], up[1]]
        for turn, shift in enumerate(mp_shifts):
            act_chunks[turn + 1] += [lax.ppermute(piece[1], "mp", shift) for piece in (down, up)]
    chunks = (grad_chunks, act_chunks)

    upper, lower, piece_sq = run_block("both", 0, meta, chunks)
    piece_sq = jnp.where(me < shared, piece_sq, 0.0)
    rows = BLK // 2
    downs, ups = [upper], [lower]

    jobs = []
    rest = {}
    roots = [None]
    for job, block in enumerate(range(shared, half_blocks), 1):
        jobs.append(lambda after, job=job, block=block: rest.__setitem__(
            block, run_block("left", job, meta, chunks, after=after)) or rest[block])
        jobs.append(lambda after, job=job, block=block: rest.__setitem__(
            block, run_block("finish", job, meta, chunks, left_root=rest[block], after=after))
            or rest[block][0])
    first = 1 + half_blocks - shared
    for position in range(per_owner):
        jobs.append(lambda after, position=position: roots.__setitem__(
            0, run_block("roots", first + position, meta, chunks, roots=roots[0],
                         position=position, count=per_owner, after=after)) or roots[0])

    def exchange(value, axis, bit):
        pairs = [(i, i ^ bit) for i in range(lax.axis_size(axis))]
        return value + lax.ppermute(value, axis, pairs)

    bits = [1 << i for i in range((owners - 1).bit_length())]
    core_bits = [1 << i for i in range((halves - 1).bit_length())]
    half_sq = piece_sq
    whole = False
    for step in range(1, owners):
        after = (downs[-1], ups[-1]) if step > 1 else ()
        down = lax.ppermute(downs[-1], "dp", ahead)
        up = lax.ppermute(ups[-1], "dp", back)
        ready = len(rest) == half_blocks - shared and len(jobs) <= per_owner
        if bits:
            half_sq = exchange(half_sq, "dp", bits.pop(0))
        elif ready and not whole:
            whole = True
            for block in rest:
                half_sq = half_sq + rest[block][2]
        elif whole and core_bits:
            half_sq = exchange(half_sq, "mp", core_bits.pop(0))
        done = jobs.pop(0)(after) if jobs else half_sq
        if step < owners - 1:
            down, up, half_sq, _ = lax.optimization_barrier((down, up, half_sq, done))
        downs.append(down)
        ups.append(up)
    while jobs:
        jobs.pop(0)((downs[-1], ups[-1]))
    while bits:
        half_sq = exchange(half_sq, "dp", bits.pop(0))
    if not whole:
        for block in rest:
            half_sq = half_sq + rest[block][2]
    while core_bits:
        half_sq = exchange(half_sq, "mp", core_bits.pop(0))
    rescale = lax.rsqrt(half_sq / (row_blocks * BLK * half_width * halves) + 1.0)

    def spot(block, lower):
        return [(block // col_blocks) * BLK + lower, (block % col_blocks) * BLK]

    early = []
    for block in range(shared, half_blocks):
        early += [(spot(jnp.int32(block), 0), rest[block][0])]
        early += [(spot(jnp.int32(block), rows), rest[block][1])]
    for step in range(owners):
        early += [(spot(jnp.minimum(from_behind[step], shared - 1), 0), downs[step])]
        early += [(spot(jnp.minimum(from_ahead[step], shared - 1), rows), ups[step])]
    late = early[-2:]
    early = early[:-2]
    canvas = None
    limit = 20
    for group in [early[i : i + limit] for i in range(0, len(early), limit)] + [late]:
        if group is late:
            tied = lax.optimization_barrier((canvas, *[piece for _, piece in late]))
            canvas = tied[0]
            group = [(where, piece) for (where, _), piece in zip(late, tied[1:])]
        spots = [value for where, _ in group for value in where]
        shape = (row_blocks * BLK, half_width)
        canvas = place_pieces(canvas, shape, spots, rescale, [piece for _, piece in group])
    return canvas, roots[0][None]


def solution(mesh):
    placed = (
        P(("member", "dp"), None),
        P(("member", "dp"), "mp"),
        P(("member", "mp"), None),
        P(("member", "mp"), None),
        P(("member", "mp"), None),
    )
    return jax.shard_map(
        on_device,
        mesh=mesh,
        in_specs=placed,
        out_specs=(P("member", "mp"), P(("member", "mp"), "dp", None, None, None)),
        check_vma=False,
    )
```

```python
import functools

import jax
import jax.numpy as jnp
from jax import lax
from jax.experimental import pallas as pl
from jax.experimental.pallas import tpu as pltpu
from jax.sharding import PartitionSpec as P


BLK = 1024
TILE = 256
ROOT_ORDERS = (2.0, 4.0)
DAMPINGS = (0.03, 0.1, 0.3, 1.0)
HBM = pltpu.MemorySpace.HBM
VMEM_LIMIT = 60 * 2**20


def table_value(picked, values_table):
    values = jnp.asarray(values_table, jnp.float32)
    matches = jnp.arange(len(values_table), dtype=jnp.int32) == picked[:, None]
    return jnp.sum(jnp.where(matches, values, 0.0), axis=1)


def wide_dot(first, second, first_dim, second_dim):
    return lax.dot_general(
        first, second, (((first_dim,), (second_dim,)), ((), ())), preferred_element_type=jnp.float32
    )


def gather_block(ints, places, sources, acts_t, grads, sems):
    owners, turns, tok, grad_refs, act_refs = sources
    turn, column = ints[0], ints[1]
    columns = pl.ds(pl.multiple_of(column * BLK, BLK), BLK)
    half_tok = tok // 2
    half_row = BLK // 2
    waits = []

    def start(copy_of, count):
        sem = sems.at[len(waits)]
        for index in range(count):
            if count == 1:
                copy_of(index, sem).start()
            else:
                pl.when(turn == index)(lambda index=index: copy_of(index, sem).start())
        waits.append(copy_of(0, sem))

    for step in range(owners):
        for way in range(2):
            if step == 0 and way == 1:
                continue
            source = places[way * owners + step]
            rows = tok if step == 0 else half_tok
            at_tok = pl.multiple_of(source * tok + (half_tok * way), half_tok)
            at_lane = pl.multiple_of(source * tok, tok)
            grad_ref = grad_refs[step * 2 + way]
            start(
                lambda _, sem, grad_ref=grad_ref, at_tok=at_tok, rows=rows: pltpu.make_async_copy(
                    grad_ref.at[:, columns], grads.at[pl.ds(at_tok, rows), :], sem
                ),
                1,
            )
            act_rows = slice(0, BLK) if step == 0 else slice(half_row * way, half_row * (way + 1))
            start(
                lambda index, sem, at_lane=at_lane, act_rows=act_rows, at=step * 2 + way: (
                    pltpu.make_async_copy(
                        act_refs[index][at], acts_t.at[act_rows, pl.ds(at_lane, tok)], sem
                    )
                ),
                turns,
            )
    for copy in waits:
        copy.wait()


def symmetric_product(matrix, second_dim, finish, outs):
    for low in range(0, BLK, TILE):
        high = low + TILE
        second = matrix[low:, :] if second_dim else matrix[:, low:]
        tile = wide_dot(matrix[low:high, :], second, 1, second_dim)
        for out, value in zip(outs, finish(tile)):
            out[low:high, low:] = value
            if high < BLK:
                out[high:, low:high] = value[:, TILE:].T


def diagonal(shape):
    return lax.broadcasted_iota(jnp.int32, shape, 0) == lax.broadcasted_iota(jnp.int32, shape, 1)


def inverse_root(side, gradient, root, square_sum, params, current, factor, raised, later):
    root_order, quartic, damping = params
    shift = damping * (square_sum / BLK + 1.0)
    scale = BLK / (2.0 * (square_sum + BLK * shift))
    inverse = 1.0 / root_order

    def first_pair(statistic):
        eye = diagonal(statistic.shape)
        scaled = jnp.where(eye, statistic + shift, statistic) * scale
        first = (jnp.where(eye, root_order + 1.0, 0.0) - scaled) * inverse
        return scaled.astype(jnp.bfloat16), first.astype(jnp.bfloat16)

    def rounded(product):
        return (product.astype(jnp.bfloat16),)

    symmetric_product(gradient.at[side], 1, first_pair, (current, factor))
    symmetric_product(factor, 0, rounded, (raised.at[0],))

    @pl.when(quartic != 0)
    def _():
        symmetric_product(raised.at[0], 0, rounded, (raised.at[1],))

    moved = wide_dot(raised[quartic], current[...], 1, 0)
    eye = diagonal(moved.shape)
    later[...] = ((jnp.where(eye, root_order + 1.0, 0.0) - moved) * inverse).astype(jnp.bfloat16)
    root[...] = wide_dot(factor[...], later[...], 1, 0).astype(jnp.bfloat16)


def block_kernel(kind, owners, turns, extra, job, position, *refs):
    refs = list(refs)
    int_table, float_table, places = refs[:3]
    ints = [int_table[4 * job + field] for field in range(4)]
    floats = [float_table[2 * job + field] for field in range(2)]
    chunks = 2 * owners - 1
    at = 3
    own = refs[at : at + chunks]
    grad_refs = [own[0], None] + own[1:]
    at += chunks
    act_refs = []
    for _ in range(turns):
        own = refs[at : at + chunks]
        act_refs.append([own[0], None] + own[1:])
        at += chunks
    tok = grad_refs[0].shape[0]
    left_in = None
    if kind == "finish":
        left_in = refs[at]
        at += 1
    at += extra
    outs = refs[at : at + (1 if kind in ("left", "roots") else 3)]
    at += len(outs)
    acts_t, grads, gradient, current, factor, raised, later, pair, sems, out_sems = refs[at:]
    gather_block(
        ints, places, (owners, turns, tok, grad_refs, act_refs), acts_t, grads, sems
    )
    block_grad = wide_dot(acts_t[...], grads[...], 1, 0)
    block_grad = jnp.where(ints[3] != 0, block_grad, 0.0).astype(jnp.bfloat16)
    gradient[0] = block_grad
    if kind != "left":
        gradient[1] = block_grad.T
    squares = block_grad.astype(jnp.float32)
    square_sum = jnp.sum(squares * squares)
    params = (floats[0], ints[2], floats[1])
    work = (current, factor, raised, later)
    if kind == "left":
        inverse_root(0, gradient, outs[0], square_sum, params, *work)
        return
    if kind == "finish":
        inverse_root(1, gradient, pair.at[1], square_sum, params, *work)
        left_root = left_in[...]
    else:

        def one_side(side, carry):
            inverse_root(side, gradient, pair.at[side], square_sum, params, *work)
            if kind == "roots":
                pltpu.make_async_copy(
                    pair.at[side], outs[0].at[position, side], out_sems.at[side]
                ).start()
            return carry

        lax.fori_loop(0, 2, one_side, 0)
        left_root = pair[0]
    if kind == "roots":
        for side in range(2):
            pltpu.make_async_copy(
                pair.at[side], outs[0].at[position, side], out_sems.at[side]
            ).wait()
        return
    later[...] = wide_dot(left_root, gradient[0], 1, 0).astype(jnp.bfloat16)
    update = wide_dot(later[...], pair[1], 1, 0).astype(jnp.bfloat16)
    outs[0][...] = update[: BLK // 2]
    outs[1][...] = update[BLK // 2 :]
    wide = update.astype(jnp.float32)
    outs[2][0, 0] = jnp.sum(wide * wide)


def run_block(kind, job, meta, chunks, left_root=None, roots=None, position=0, count=1, after=()):
    ints, floats, places = meta
    grad_chunks, act_chunks = chunks
    owners = (len(grad_chunks) + 1) // 2
    turns = len(act_chunks)
    tokens = owners * grad_chunks[0].shape[0]
    smem = pl.BlockSpec(memory_space=pltpu.SMEM)
    vmem = pl.BlockSpec(memory_space=pltpu.VMEM)
    hbm = pl.BlockSpec(memory_space=HBM)
    operands = [ints, floats, places, *grad_chunks]
    for turn in act_chunks:
        operands += turn
    specs = [smem] * 3 + [hbm] * (len(operands) - 3)
    if left_root is not None:
        operands.append(left_root)
        specs.append(vmem)
    aliases = {}
    if roots is not None:
        aliases = {len(operands): 0}
        after = (roots, *after)
    operands += after
    specs += [hbm] * len(after)
    half = jnp.bfloat16
    piece = jax.ShapeDtypeStruct((BLK // 2, BLK), half)
    if kind == "left":
        out_shape, out_specs = jax.ShapeDtypeStruct((BLK, BLK), half), vmem
    elif kind == "roots":
        out_shape, out_specs = jax.ShapeDtypeStruct((count, 2, BLK, BLK), half), hbm
    else:
        out_shape = (piece, piece, jax.ShapeDtypeStruct((1, 1), jnp.float32))
        out_specs = (vmem, vmem, smem)
    matmuls = {"left": 6, "roots": 11, "finish": 8, "both": 13}[kind]
    return pl.pallas_call(
        functools.partial(block_kernel, kind, owners, turns, len(after), job, position),
        out_shape=out_shape,
        in_specs=specs,
        out_specs=out_specs,
        input_output_aliases=aliases,
        scratch_shapes=[
            pltpu.VMEM((BLK, tokens), half),
            pltpu.VMEM((tokens, BLK), half),
            pltpu.VMEM((2, BLK, BLK), half),
            pltpu.VMEM((BLK, BLK), half),
            pltpu.VMEM((BLK, BLK), half),
            pltpu.VMEM((2, BLK, BLK), half),
            pltpu.VMEM((BLK, BLK), half),
            pltpu.VMEM((2, BLK, BLK), half),
            pltpu.SemaphoreType.DMA((2 * (2 * owners - 1),)),
            pltpu.SemaphoreType.DMA((2,)),
        ],
        compiler_params=pltpu.CompilerParams(vmem_limit_bytes=VMEM_LIMIT),
        cost_estimate=pl.CostEstimate(
            flops=matmuls * 2 * BLK**3, bytes_accessed=6 * 2 * BLK**2, transcendentals=0
        ),
    )(*operands)


def place_kernel(first, count, extra, *refs):
    spots, rescale = refs[:2]
    pieces = refs[2 : 2 + count]
    canvas, held, in_sems, out_sems = refs[2 + count + extra :]
    rows = held.shape[1]
    loads = []
    stores = []
    for index in range(count):
        row = pl.multiple_of(spots[2 * (first + index)], rows)
        column = pl.multiple_of(spots[2 * (first + index) + 1], BLK)
        loads.append(pltpu.make_async_copy(pieces[index], held.at[index], in_sems.at[index]))
        stores.append(
            pltpu.make_async_copy(
                held.at[index],
                canvas.at[pl.ds(row, rows), pl.ds(column, BLK)],
                out_sems.at[index],
            )
        )
    for load in loads:
        load.start()
    for index in range(count):
        loads[index].wait()
        wide = held[index].astype(jnp.float32) * rescale[0, 0]
        held[index] = wide.astype(jnp.bfloat16)
        stores[index].start()
    for store in stores:
        store.wait()


def place_pieces(canvas, shape, spots, first, rescale, pieces):
    count = len(pieces)
    smem = pl.BlockSpec(memory_space=pltpu.SMEM)
    hbm = pl.BlockSpec(memory_space=HBM)
    old = [] if canvas is None else [canvas]
    return pl.pallas_call(
        functools.partial(place_kernel, first, count, len(old)),
        out_shape=jax.ShapeDtypeStruct(shape, jnp.bfloat16),
        in_specs=[smem, smem] + [hbm] * (count + len(old)),
        out_specs=hbm,
        input_output_aliases={2 + count: 0} if old else {},
        scratch_shapes=[
            pltpu.VMEM((count, *pieces[0].shape), jnp.bfloat16),
            pltpu.SemaphoreType.DMA((count,)),
            pltpu.SemaphoreType.DMA((count,)),
        ],
        compiler_params=pltpu.CompilerParams(vmem_limit_bytes=VMEM_LIMIT),
        cost_estimate=pl.CostEstimate(
            flops=count * BLK * BLK * 100, bytes_accessed=2 * count * BLK * BLK, transcendentals=0
        ),
        name="place",
    )(spots, rescale, *pieces, *old)


def ring_pairs(count):
    order = list(range(0, count, 2)) + list(range(1, count, 2))[::-1]
    ahead = [(order[i], order[(i + 1) % count]) for i in range(count)]
    back = [(b, a) for a, b in ahead]
    return order, ahead, back


def shampoo_step(activations, out_grads, slot_table, exponent_index, damping_index):
    tok_count = activations.shape[0]
    row_blocks = activations.shape[1] // BLK
    half_width = out_grads.shape[1]
    col_blocks = half_width // BLK
    half_blocks = row_blocks * col_blocks
    owners = lax.axis_size("dp")
    halves = lax.axis_size("mp")
    me = lax.axis_index("dp")
    core = lax.axis_index("mp")
    slot_count = slot_table.shape[1]
    per_owner = slot_count // owners
    order, ahead, back = ring_pairs(owners)
    order_of = jnp.asarray(order, jnp.int32)
    place = jnp.asarray([order.index(i) for i in range(owners)], jnp.int32)[me]
    steps = jnp.arange(owners, dtype=jnp.int32)
    from_behind = order_of[(place - steps) % owners]
    from_ahead = order_of[(place + steps) % owners]
    places = jnp.concatenate([from_behind, from_ahead])

    table = slot_table[0, :half_blocks]
    exponents = exponent_index[0]
    dampings = damping_index[0]

    shared = min(owners, half_blocks)
    mine = jnp.minimum(me, shared - 1)
    block_range = jnp.arange(half_blocks, dtype=jnp.int32)
    slot_range = jnp.arange(slot_count, dtype=jnp.int32)
    spread = jnp.concatenate([mine[None], block_range[shared:]])
    spread_slots = jnp.sum(
        jnp.where(spread[:, None] == block_range[None, :], table[None, :], 0), axis=1
    )
    own_slots = me * per_owner + jnp.arange(per_owner, dtype=jnp.int32)
    matches = own_slots[:, None] == table[None, :]
    own_blocks = jnp.sum(jnp.where(matches, block_range[None, :], 0), axis=1)
    blocks = jnp.concatenate([spread, own_blocks])
    slots = jnp.concatenate([spread_slots, own_slots])
    filled = jnp.concatenate([jnp.ones_like(spread), jnp.any(matches, axis=1).astype(jnp.int32)])
    at_slot = slots[:, None] == slot_range[None, :]
    exp_picks = jnp.sum(jnp.where(at_slot, exponents[None, :], 0), axis=1)
    damp_picks = jnp.sum(jnp.where(at_slot, dampings[None, :], 0), axis=1)
    turn = (core - blocks // col_blocks) % halves
    ints = jnp.stack([turn, blocks % col_blocks, exp_picks, filled], axis=1).reshape(-1)
    floats = jnp.stack(
        [table_value(exp_picks, ROOT_ORDERS), table_value(damp_picks, DAMPINGS)], axis=1
    ).reshape(-1)
    late_count = 2
    rows = BLK // 2
    put_blocks = jnp.concatenate(
        [jnp.repeat(block_range[shared:], 2), jnp.stack([from_behind, from_ahead], 1).reshape(-1)]
    )
    put_blocks = jnp.minimum(put_blocks, half_blocks - 1)
    put_lower = jnp.tile(jnp.asarray([0, rows], jnp.int32), put_blocks.shape[0] // 2)
    spots = jnp.stack(
        [(put_blocks // col_blocks) * BLK + put_lower, (put_blocks % col_blocks) * BLK], axis=1
    ).reshape(-1)
    meta = (ints.astype(jnp.int32), floats, places, spots)

    part = activations.shape[1] // halves
    assert part == BLK
    act_part = lax.dynamic_slice(activations, (0, core * part), (tok_count, part)).T
    mp_shifts = [[(i, (i + s) % halves) for i in range(halves)] for s in range(1, halves)]
    half_tok = tok_count // 2
    half_row = part // 2

    grad_chunks = [out_grads]
    act_chunks = [[act_part]]
    for shift in mp_shifts:
        act_chunks.append([lax.ppermute(act_part, "mp", shift)])
    down = (out_grads[:half_tok], act_part[:half_row])
    up = (out_grads[half_tok:], act_part[half_row:])
    for step in range(1, owners):
        down = tuple(lax.ppermute(piece, "dp", ahead) for piece in down)
        up = tuple(lax.ppermute(piece, "dp", back) for piece in up)
        if step == 2:
            down, up, meta = lax.optimization_barrier((down, up, meta))
        else:
            down, up = lax.optimization_barrier((down, up))
        grad_chunks += [down[0], up[0]]
        act_chunks[0] += [down[1], up[1]]
        for turn, shift in enumerate(mp_shifts):
            act_chunks[turn + 1] += [lax.ppermute(piece[1], "mp", shift) for piece in (down, up)]
    chunks = (grad_chunks, act_chunks)

    spots = meta[3]
    meta = meta[:3]
    upper, lower, piece_sq = run_block("both", 0, meta, chunks)
    piece_sq = jnp.where(me < shared, piece_sq, 0.0)
    downs, ups = [upper], [lower]

    jobs = []
    rest = {}
    roots = [None]
    for job, block in enumerate(range(shared, half_blocks), 1):
        jobs.append(("left", lambda after, job=job, block=block: rest.__setitem__(
            block, run_block("left", job, meta, chunks, after=after)) or rest[block]))
        jobs.append(("finish", lambda after, job=job, block=block: rest.__setitem__(
            block, run_block("finish", job, meta, chunks, left_root=rest[block], after=after))
            or rest[block][0]))
    first = 1 + half_blocks - shared
    for position in range(per_owner):
        jobs.append(("roots", lambda after, position=position: roots.__setitem__(
            0, run_block("roots", first + position, meta, chunks, roots=roots[0],
                         position=position, count=per_owner, after=after)) or roots[0]))

    def exchange(value, axis, bit):
        pairs = [(i, i ^ bit) for i in range(lax.axis_size(axis))]
        return value + lax.ppermute(value, axis, pairs)

    bits = [1 << i for i in range((owners - 1).bit_length())]
    core_bits = [1 << i for i in range((halves - 1).bit_length())]
    half_sq = piece_sq
    for step in range(1, owners):
        after = (downs[-1], ups[-1]) if step > 1 else ()
        down = lax.ppermute(downs[-1], "dp", ahead)
        up = lax.ppermute(ups[-1], "dp", back)
        kind = jobs[0][0] if jobs else None
        done = jobs.pop(0)[1](after) if jobs else half_sq
        if kind == "left" and bits:
            half_sq, done = lax.optimization_barrier((half_sq, done))
            for bit in bits[:2]:
                half_sq = exchange(half_sq, "dp", bit)
            bits = bits[2:]
        if step < owners - 1:
            down, up, half_sq, _ = lax.optimization_barrier((down, up, half_sq, done))
        downs.append(down)
        ups.append(up)
    while jobs:
        jobs.pop(0)[1]((downs[-1], ups[-1]))
    while bits:
        half_sq = exchange(half_sq, "dp", bits.pop(0))
    for block in rest:
        half_sq = half_sq + rest[block][2]
    while core_bits:
        half_sq = exchange(half_sq, "mp", core_bits.pop(0))
    rescale = lax.rsqrt(half_sq / (row_blocks * BLK * half_width * halves) + 1.0)

    pieces = []
    for block in rest:
        pieces += rest[block][:2]
    for down, up in zip(downs, ups):
        pieces += [down, up]
    canvas = None
    limit = 20
    shape = (row_blocks * BLK, half_width)
    early = len(pieces) - late_count
    cuts = [*range(0, early, limit), early, len(pieces)]
    for low, high in zip(cuts[:-1], cuts[1:]):
        group = pieces[low:high]
        canvas = place_pieces(canvas, shape, spots, low, rescale, group)
    return canvas, roots[0][None]


def solution(mesh):
    placed = (
        P(("member", "dp"), None),
        P(("member", "dp"), "mp"),
        P(("member", "mp"), None),
        P(("member", "mp"), None),
        P(("member", "mp"), None),
    )
    return jax.shard_map(
        shampoo_step,
        mesh=mesh,
        in_specs=placed,
        out_specs=(P("member", "mp"), P(("member", "mp"), "dp", None, None, None)),
        check_vma=False,
    )
```

```python
import functools

import jax
import jax.numpy as jnp
from jax import lax
from jax.experimental import pallas as pl
from jax.experimental.pallas import tpu as pltpu
from jax.sharding import PartitionSpec as P


BLK = 1024
TILE = 256
ROOT_ORDERS = (2.0, 4.0)
DAMPINGS = (0.03, 0.1, 0.3, 1.0)
HBM = pltpu.MemorySpace.HBM
VMEM_LIMIT = 60 * 2**20


def table_value(picked, values_table):
    values = jnp.asarray(values_table, jnp.float32)
    matches = jnp.arange(len(values_table), dtype=jnp.int32) == picked[:, None]
    return jnp.sum(jnp.where(matches, values, 0.0), axis=1)


def wide_dot(first, second, first_dim, second_dim):
    return lax.dot_general(
        first, second, (((first_dim,), (second_dim,)), ((), ())), preferred_element_type=jnp.float32
    )


def gather_block(ints, places, sources, acts_t, grads, sems):
    owners, turns, tok, grad_refs, act_refs = sources
    turn, column = ints[0], ints[1]
    columns = pl.ds(pl.multiple_of(column * BLK, BLK), BLK)
    half_tok = tok // 2
    half_row = BLK // 2
    waits = []

    def start(copy_of, count):
        sem = sems.at[len(waits)]
        for index in range(count):
            if count == 1:
                copy_of(index, sem).start()
            else:
                pl.when(turn == index)(lambda index=index: copy_of(index, sem).start())
        waits.append(copy_of(0, sem))

    for step in range(owners):
        for way in range(2):
            if step == 0 and way == 1:
                continue
            source = places[way * owners + step]
            rows = tok if step == 0 else half_tok
            at_tok = pl.multiple_of(source * tok + (half_tok * way), half_tok)
            at_lane = pl.multiple_of(source * tok, tok)
            grad_ref = grad_refs[step * 2 + way]
            start(
                lambda _, sem, grad_ref=grad_ref, at_tok=at_tok, rows=rows: pltpu.make_async_copy(
                    grad_ref.at[:, columns], grads.at[pl.ds(at_tok, rows), :], sem
                ),
                1,
            )
            act_rows = slice(0, BLK) if step == 0 else slice(half_row * way, half_row * (way + 1))
            start(
                lambda index, sem, at_lane=at_lane, act_rows=act_rows, at=step * 2 + way: (
                    pltpu.make_async_copy(
                        act_refs[index][at], acts_t.at[act_rows, pl.ds(at_lane, tok)], sem
                    )
                ),
                turns,
            )
    for copy in waits:
        copy.wait()


def symmetric_product(matrix, second_dim, finish, outs):
    for low in range(0, BLK, TILE):
        high = low + TILE
        second = matrix[low:, :] if second_dim else matrix[:, low:]
        tile = wide_dot(matrix[low:high, :], second, 1, second_dim)
        for out, value in zip(outs, finish(tile)):
            out[low:high, low:] = value
            if high < BLK:
                out[high:, low:high] = value[:, TILE:].T


def diagonal(shape):
    return lax.broadcasted_iota(jnp.int32, shape, 0) == lax.broadcasted_iota(jnp.int32, shape, 1)


def inverse_root(side, gradient, root, square_sum, params, current, factor, raised, later):
    root_order, quartic, damping = params
    shift = damping * (square_sum / BLK + 1.0)
    scale = BLK / (2.0 * (square_sum + BLK * shift))
    inverse = 1.0 / root_order

    def first_pair(statistic):
        eye = diagonal(statistic.shape)
        scaled = jnp.where(eye, statistic + shift, statistic) * scale
        first = (jnp.where(eye, root_order + 1.0, 0.0) - scaled) * inverse
        return scaled.astype(jnp.bfloat16), first.astype(jnp.bfloat16)

    def rounded(product):
        return (product.astype(jnp.bfloat16),)

    symmetric_product(gradient.at[side], 1, first_pair, (current, factor))
    symmetric_product(factor, 0, rounded, (raised.at[0],))

    @pl.when(quartic != 0)
    def _():
        symmetric_product(raised.at[0], 0, rounded, (raised.at[1],))

    moved = wide_dot(raised[quartic], current[...], 1, 0)
    eye = diagonal(moved.shape)
    later[...] = ((jnp.where(eye, root_order + 1.0, 0.0) - moved) * inverse).astype(jnp.bfloat16)
    root[...] = wide_dot(factor[...], later[...], 1, 0).astype(jnp.bfloat16)


def block_kernel(kind, owners, turns, extra, job, position, *refs):
    refs = list(refs)
    int_table, float_table, places = refs[:3]
    ints = [int_table[4 * job + field] for field in range(4)]
    floats = [float_table[2 * job + field] for field in range(2)]
    chunks = 2 * owners - 1
    at = 3
    own = refs[at : at + chunks]
    grad_refs = [own[0], None] + own[1:]
    at += chunks
    act_refs = []
    for _ in range(turns):
        own = refs[at : at + chunks]
        act_refs.append([own[0], None] + own[1:])
        at += chunks
    tok = grad_refs[0].shape[0]
    left_in = None
    if kind == "finish":
        left_in = refs[at]
        at += 1
    at += extra
    outs = refs[at : at + (1 if kind in ("left", "roots") else 3)]
    at += len(outs)
    acts_t, grads, gradient, current, factor, raised, later, pair, sems, out_sems = refs[at:]
    gather_block(
        ints, places, (owners, turns, tok, grad_refs, act_refs), acts_t, grads, sems
    )
    block_grad = wide_dot(acts_t[...], grads[...], 1, 0)
    block_grad = jnp.where(ints[3] != 0, block_grad, 0.0).astype(jnp.bfloat16)
    gradient[0] = block_grad
    if kind != "left":
        gradient[1] = block_grad.T
    squares = block_grad.astype(jnp.float32)
    square_sum = jnp.sum(squares * squares)
    params = (floats[0], ints[2], floats[1])
    work = (current, factor, raised, later)
    if kind == "left":
        inverse_root(0, gradient, outs[0], square_sum, params, *work)
        return
    if kind == "finish":
        inverse_root(1, gradient, pair.at[1], square_sum, params, *work)
        left_root = left_in[...]
    else:

        def one_side(side, carry):
            inverse_root(side, gradient, pair.at[side], square_sum, params, *work)
            if kind == "roots":
                pltpu.make_async_copy(
                    pair.at[side], outs[0].at[position, side], out_sems.at[side]
                ).start()
            return carry

        lax.fori_loop(0, 2, one_side, 0)
        left_root = pair[0]
    if kind == "roots":
        for side in range(2):
            pltpu.make_async_copy(
                pair.at[side], outs[0].at[position, side], out_sems.at[side]
            ).wait()
        return
    later[...] = wide_dot(left_root, gradient[0], 1, 0).astype(jnp.bfloat16)
    update = wide_dot(later[...], pair[1], 1, 0).astype(jnp.bfloat16)
    outs[0][...] = update[: BLK // 2]
    outs[1][...] = update[BLK // 2 :]
    wide = update.astype(jnp.float32)
    outs[2][0, 0] = jnp.sum(wide * wide)


def run_block(kind, job, meta, chunks, left_root=None, roots=None, position=0, count=1, after=()):
    ints, floats, places = meta
    grad_chunks, act_chunks = chunks
    owners = (len(grad_chunks) + 1) // 2
    turns = len(act_chunks)
    tokens = owners * grad_chunks[0].shape[0]
    smem = pl.BlockSpec(memory_space=pltpu.SMEM)
    vmem = pl.BlockSpec(memory_space=pltpu.VMEM)
    hbm = pl.BlockSpec(memory_space=HBM)
    operands = [ints, floats, places, *grad_chunks]
    for turn in act_chunks:
        operands += turn
    specs = [smem] * 3 + [hbm] * (len(operands) - 3)
    if left_root is not None:
        operands.append(left_root)
        specs.append(vmem)
    aliases = {}
    if roots is not None:
        aliases = {len(operands): 0}
        after = (roots, *after)
    operands += after
    specs += [hbm] * len(after)
    half = jnp.bfloat16
    piece = jax.ShapeDtypeStruct((BLK // 2, BLK), half)
    if kind == "left":
        out_shape, out_specs = jax.ShapeDtypeStruct((BLK, BLK), half), vmem
    elif kind == "roots":
        out_shape, out_specs = jax.ShapeDtypeStruct((count, 2, BLK, BLK), half), hbm
    else:
        out_shape = (piece, piece, jax.ShapeDtypeStruct((1, 1), jnp.float32))
        out_specs = (vmem, vmem, smem)
    matmuls = {"left": 6, "roots": 11, "finish": 8, "both": 13}[kind]
    return pl.pallas_call(
        functools.partial(block_kernel, kind, owners, turns, len(after), job, position),
        out_shape=out_shape,
        in_specs=specs,
        out_specs=out_specs,
        input_output_aliases=aliases,
        scratch_shapes=[
            pltpu.VMEM((BLK, tokens), half),
            pltpu.VMEM((tokens, BLK), half),
            pltpu.VMEM((2, BLK, BLK), half),
            pltpu.VMEM((BLK, BLK), half),
            pltpu.VMEM((BLK, BLK), half),
            pltpu.VMEM((2, BLK, BLK), half),
            pltpu.VMEM((BLK, BLK), half),
            pltpu.VMEM((2, BLK, BLK), half),
            pltpu.SemaphoreType.DMA((2 * (2 * owners - 1),)),
            pltpu.SemaphoreType.DMA((2,)),
        ],
        compiler_params=pltpu.CompilerParams(vmem_limit_bytes=VMEM_LIMIT),
        cost_estimate=pl.CostEstimate(
            flops=matmuls * 2 * BLK**3, bytes_accessed=6 * 2 * BLK**2, transcendentals=0
        ),
    )(*operands)


def place_kernel(first, count, late_count, extra, *refs):
    spots, rescale = refs[:2]
    pieces = refs[2 : 2 + count]
    canvas, held, in_sems, out_sems = refs[2 + count + extra :]
    near = late_count > 0
    rows = held.shape[1]
    loads = []
    stores = []
    for index in range(count):
        row = pl.multiple_of(spots[2 * (first + index)], rows)
        column = pl.multiple_of(spots[2 * (first + index) + 1], BLK)
        if not near:
            loads.append(pltpu.make_async_copy(pieces[index], held.at[index], in_sems.at[index]))
        stores.append(
            pltpu.make_async_copy(
                held.at[index],
                canvas.at[pl.ds(row, rows), pl.ds(column, BLK)],
                out_sems.at[index],
            )
        )
    if not near:
        for load in loads:
            load.start()
    for index in range(count):
        if not near:
            loads[index].wait()
        piece = pieces[index] if near else held.at[index]
        wide = piece[...].astype(jnp.float32) * rescale[0, 0]
        held[index] = wide.astype(jnp.bfloat16)
        stores[index].start()
    for store in stores:
        store.wait()


def place_pieces(canvas, shape, spots, first, rescale, pieces, late_count=0):
    count = len(pieces)
    smem = pl.BlockSpec(memory_space=pltpu.SMEM)
    hbm = pl.BlockSpec(memory_space=HBM)
    vmem = pl.BlockSpec(memory_space=pltpu.VMEM)
    old = [] if canvas is None else [canvas]
    return pl.pallas_call(
        functools.partial(place_kernel, first, count, late_count, len(old)),
        out_shape=jax.ShapeDtypeStruct(shape, jnp.bfloat16),
        in_specs=[smem, smem] + [vmem if late_count else hbm] * count + [hbm] * len(old),
        out_specs=hbm,
        input_output_aliases={2 + count: 0} if old else {},
        scratch_shapes=[
            pltpu.VMEM((count, *pieces[0].shape), jnp.bfloat16),
            pltpu.SemaphoreType.DMA((count,)),
            pltpu.SemaphoreType.DMA((count,)),
        ],
        compiler_params=pltpu.CompilerParams(vmem_limit_bytes=VMEM_LIMIT),
        cost_estimate=pl.CostEstimate(
            flops=count * BLK * BLK * 100, bytes_accessed=2 * count * BLK * BLK, transcendentals=0
        ),
        name="place",
    )(spots, rescale, *pieces, *old)


def ring_pairs(count):
    order = list(range(0, count, 2)) + list(range(1, count, 2))[::-1]
    ahead = [(order[i], order[(i + 1) % count]) for i in range(count)]
    back = [(b, a) for a, b in ahead]
    return order, ahead, back


def sum_steps(owners):
    bits = [1 << i for i in range((owners - 1).bit_length())]
    return dict(zip([0, 1, 3, 4, 2, *range(5, owners)], bits))


def shampoo_step(activations, out_grads, slot_table, exponent_index, damping_index):
    tok_count = activations.shape[0]
    row_blocks = activations.shape[1] // BLK
    half_width = out_grads.shape[1]
    col_blocks = half_width // BLK
    half_blocks = row_blocks * col_blocks
    owners = lax.axis_size("dp")
    halves = lax.axis_size("mp")
    me = lax.axis_index("dp")
    core = lax.axis_index("mp")
    slot_count = slot_table.shape[1]
    per_owner = slot_count // owners
    order, ahead, back = ring_pairs(owners)
    order_of = jnp.asarray(order, jnp.int32)
    place = jnp.asarray([order.index(i) for i in range(owners)], jnp.int32)[me]
    steps = jnp.arange(owners, dtype=jnp.int32)
    from_behind = order_of[(place - steps) % owners]
    from_ahead = order_of[(place + steps) % owners]
    places = jnp.concatenate([from_behind, from_ahead])

    table = slot_table[0, :half_blocks]
    exponents = exponent_index[0]
    dampings = damping_index[0]

    shared = min(owners, half_blocks)
    mine = jnp.minimum(me, shared - 1)
    block_range = jnp.arange(half_blocks, dtype=jnp.int32)
    slot_range = jnp.arange(slot_count, dtype=jnp.int32)
    spread = jnp.concatenate([mine[None], block_range[shared:]])
    spread_slots = jnp.sum(
        jnp.where(spread[:, None] == block_range[None, :], table[None, :], 0), axis=1
    )
    own_slots = me * per_owner + jnp.arange(per_owner, dtype=jnp.int32)
    matches = own_slots[:, None] == table[None, :]
    own_blocks = jnp.sum(jnp.where(matches, block_range[None, :], 0), axis=1)
    blocks = jnp.concatenate([spread, own_blocks])
    slots = jnp.concatenate([spread_slots, own_slots])
    filled = jnp.concatenate([jnp.ones_like(spread), jnp.any(matches, axis=1).astype(jnp.int32)])
    at_slot = slots[:, None] == slot_range[None, :]
    exp_picks = jnp.sum(jnp.where(at_slot, exponents[None, :], 0), axis=1)
    damp_picks = jnp.sum(jnp.where(at_slot, dampings[None, :], 0), axis=1)
    turn = (core - blocks // col_blocks) % halves
    ints = jnp.stack([turn, blocks % col_blocks, exp_picks, filled], axis=1).reshape(-1)
    floats = jnp.stack(
        [table_value(exp_picks, ROOT_ORDERS), table_value(damp_picks, DAMPINGS)], axis=1
    ).reshape(-1)
    late_count = 2
    rows = BLK // 2
    put_blocks = jnp.concatenate(
        [jnp.repeat(block_range[shared:], 2), jnp.stack([from_behind, from_ahead], 1).reshape(-1)]
    )
    put_blocks = jnp.minimum(put_blocks, half_blocks - 1)
    put_lower = jnp.tile(jnp.asarray([0, rows], jnp.int32), put_blocks.shape[0] // 2)
    spots = jnp.stack(
        [(put_blocks // col_blocks) * BLK + put_lower, (put_blocks % col_blocks) * BLK], axis=1
    ).reshape(-1)
    meta = (ints.astype(jnp.int32), floats, places, spots)

    part = activations.shape[1] // halves
    assert part == BLK
    act_part = lax.dynamic_slice(activations, (0, core * part), (tok_count, part)).T
    mp_shifts = [[(i, (i + s) % halves) for i in range(halves)] for s in range(1, halves)]
    half_tok = tok_count // 2
    half_row = part // 2

    grad_chunks = [out_grads]
    act_chunks = [[act_part]]
    for shift in mp_shifts:
        act_chunks.append([lax.ppermute(act_part, "mp", shift)])
    down, up = out_grads[:half_tok], out_grads[half_tok:]
    acts = (act_part[:half_row], act_part[half_row:])
    for step in range(1, owners):
        down = lax.ppermute(down, "dp", ahead)
        up = lax.ppermute(up, "dp", back)
        for act_step in (1, 2) if step == 1 else (step + 1,):
            if act_step < owners:
                acts = (lax.ppermute(acts[0], "dp", ahead), lax.ppermute(acts[1], "dp", back))
                act_chunks[0] += acts
                for turn, shift in enumerate(mp_shifts):
                    act_chunks[turn + 1] += [lax.ppermute(piece, "mp", shift) for piece in acts]
        if step == 2:
            down, up, acts, meta = lax.optimization_barrier((down, up, acts, meta))
        else:
            down, up, acts = lax.optimization_barrier((down, up, acts))
        grad_chunks += [down, up]
    chunks = (grad_chunks, act_chunks)

    spots = meta[3]
    meta = meta[:3]
    upper, lower, piece_sq = run_block("both", 0, meta, chunks)
    piece_sq = jnp.where(me < shared, piece_sq, 0.0)
    downs, ups = [upper], [lower]

    jobs = []
    rest = {}
    roots = [None]
    for job, block in enumerate(range(shared, half_blocks), 1):
        jobs.append(("left", lambda after, job=job, block=block: rest.__setitem__(
            block, run_block("left", job, meta, chunks, after=after)) or rest[block]))
        jobs.append(("finish", lambda after, job=job, block=block: rest.__setitem__(
            block, run_block("finish", job, meta, chunks, left_root=rest[block], after=after))
            or rest[block][0]))
    first = 1 + half_blocks - shared
    for position in range(per_owner):
        jobs.append(("roots", lambda after, position=position: roots.__setitem__(
            0, run_block("roots", first + position, meta, chunks, roots=roots[0],
                         position=position, count=per_owner, after=after)) or roots[0]))

    def exchange(value, axis, bit):
        pairs = [(i, i ^ bit) for i in range(lax.axis_size(axis))]
        return value + lax.ppermute(value, axis, pairs)

    half_sq = piece_sq
    sums = sum_steps(owners)
    if 0 in sums:
        half_sq = exchange(half_sq, "dp", sums[0])
        upper, lower, half_sq = lax.optimization_barrier((upper, lower, half_sq))
        downs, ups = [upper], [lower]
    for step in range(1, owners):
        after = (downs[-1], ups[-1]) if step > 1 else ()
        down = lax.ppermute(downs[-1], "dp", ahead)
        up = lax.ppermute(ups[-1], "dp", back)
        done = jobs.pop(0)[1](after) if jobs else half_sq
        if step in sums:
            half_sq, done = lax.optimization_barrier((half_sq, done))
            half_sq = exchange(half_sq, "dp", sums[step])
        if step < owners - 1:
            down, up, half_sq, _ = lax.optimization_barrier((down, up, half_sq, done))
        downs.append(down)
        ups.append(up)
    while jobs:
        jobs.pop(0)[1]((downs[-1], ups[-1]))
    for block in rest:
        half_sq = half_sq + rest[block][2]
    for bit in [1 << i for i in range((halves - 1).bit_length())]:
        half_sq = exchange(half_sq, "mp", bit)
    rescale = lax.rsqrt(half_sq / (row_blocks * BLK * half_width * halves) + 1.0)

    pieces = []
    for block in rest:
        pieces += rest[block][:2]
    for down, up in zip(downs, ups):
        pieces += [down, up]
    canvas = None
    limit = 20
    shape = (row_blocks * BLK, half_width)
    early = len(pieces) - late_count
    cuts = [*range(0, early, limit), early, len(pieces)]
    for low, high in zip(cuts[:-1], cuts[1:]):
        group = pieces[low:high]
        late = late_count if low == early else 0
        canvas = place_pieces(canvas, shape, spots, low, rescale, group, late)
    return canvas, roots[0][None]


def solution(mesh):
    placed = (
        P(("member", "dp"), None),
        P(("member", "dp"), "mp"),
        P(("member", "mp"), None),
        P(("member", "mp"), None),
        P(("member", "mp"), None),
    )
    return jax.shard_map(
        shampoo_step,
        mesh=mesh,
        in_specs=placed,
        out_specs=(P("member", "mp"), P(("member", "mp"), "dp", None, None, None)),
        check_vma=False,
    )
```

```python
import functools

import jax
import jax.numpy as jnp
from jax import lax
from jax.experimental import pallas as pl
from jax.experimental.pallas import tpu as pltpu
from jax.sharding import PartitionSpec as P


BLK = 1024
TILE = 256
ROOT_ORDERS = (2.0, 4.0)
DAMPINGS = (0.03, 0.1, 0.3, 1.0)
HBM = pltpu.MemorySpace.HBM
VMEM_LIMIT = 60 * 2**20


def table_value(picked, values_table):
    values = jnp.asarray(values_table, jnp.float32)
    matches = jnp.arange(len(values_table), dtype=jnp.int32) == picked[:, None]
    return jnp.sum(jnp.where(matches, values, 0.0), axis=1)


def wide_dot(first, second, first_dim, second_dim):
    return lax.dot_general(
        first, second, (((first_dim,), (second_dim,)), ((), ())), preferred_element_type=jnp.float32
    )


def gather_block(ints, places, sources, acts_t, grads, sems):
    owners, turns, tok, grad_refs, act_refs = sources
    turn, column = ints[0], ints[1]
    columns = pl.ds(pl.multiple_of(column * BLK, BLK), BLK)
    half_tok = tok // 2
    half_row = BLK // 2
    waits = []

    def start(copy_of, count):
        sem = sems.at[len(waits)]
        for index in range(count):
            if count == 1:
                copy_of(index, sem).start()
            else:
                pl.when(turn == index)(lambda index=index: copy_of(index, sem).start())
        waits.append(copy_of(0, sem))

    for step in range(owners):
        for way in range(2):
            if step == 0 and way == 1:
                continue
            source = places[way * owners + step]
            rows = tok if step == 0 else half_tok
            at_tok = pl.multiple_of(source * tok + (half_tok * way), half_tok)
            at_lane = pl.multiple_of(source * tok, tok)
            grad_ref = grad_refs[step * 2 + way]
            start(
                lambda _, sem, grad_ref=grad_ref, at_tok=at_tok, rows=rows: pltpu.make_async_copy(
                    grad_ref.at[:, columns], grads.at[pl.ds(at_tok, rows), :], sem
                ),
                1,
            )
            act_rows = slice(0, BLK) if step == 0 else slice(half_row * way, half_row * (way + 1))
            start(
                lambda index, sem, at_lane=at_lane, act_rows=act_rows, at=step * 2 + way: (
                    pltpu.make_async_copy(
                        act_refs[index][at], acts_t.at[act_rows, pl.ds(at_lane, tok)], sem
                    )
                ),
                turns,
            )
    for copy in waits:
        copy.wait()


def symmetric_product(matrix, second_dim, finish, outs):
    for low in range(0, BLK, TILE):
        high = low + TILE
        second = matrix[low:, :] if second_dim else matrix[:, low:]
        tile = wide_dot(matrix[low:high, :], second, 1, second_dim)
        for out, value in zip(outs, finish(tile)):
            out[low:high, low:] = value
            if high < BLK:
                out[high:, low:high] = value[:, TILE:].T


def diagonal(shape):
    return lax.broadcasted_iota(jnp.int32, shape, 0) == lax.broadcasted_iota(jnp.int32, shape, 1)


def inverse_root(side, gradient, root, square_sum, params, current, factor, raised, later):
    root_order, quartic, damping = params
    shift = damping * (square_sum / BLK + 1.0)
    scale = BLK / (2.0 * (square_sum + BLK * shift))
    inverse = 1.0 / root_order

    def first_pair(statistic):
        eye = diagonal(statistic.shape)
        scaled = jnp.where(eye, statistic + shift, statistic) * scale
        first = (jnp.where(eye, root_order + 1.0, 0.0) - scaled) * inverse
        return scaled.astype(jnp.bfloat16), first.astype(jnp.bfloat16)

    def rounded(product):
        return (product.astype(jnp.bfloat16),)

    symmetric_product(gradient.at[side], 1, first_pair, (current, factor))
    symmetric_product(factor, 0, rounded, (raised.at[0],))

    @pl.when(quartic != 0)
    def _():
        symmetric_product(raised.at[0], 0, rounded, (raised.at[1],))

    moved = wide_dot(raised[quartic], current[...], 1, 0)
    later[...] = (moved * -inverse).astype(jnp.bfloat16)
    for low in range(0, BLK, TILE):
        near = slice(low, low + TILE)
        tile = moved[near, near]
        eye = diagonal(tile.shape)
        tile = (jnp.where(eye, root_order + 1.0, 0.0) - tile) * inverse
        later[near, near] = tile.astype(jnp.bfloat16)
    root[...] = wide_dot(factor[...], later[...], 1, 0).astype(jnp.bfloat16)


def block_kernel(kind, owners, turns, extra, job, position, *refs):
    refs = list(refs)
    int_table, float_table, places = refs[:3]
    ints = [int_table[4 * job + field] for field in range(4)]
    floats = [float_table[2 * job + field] for field in range(2)]
    chunks = 2 * owners - 1
    at = 3
    own = refs[at : at + chunks]
    grad_refs = [own[0], None] + own[1:]
    at += chunks
    act_refs = []
    for _ in range(turns):
        own = refs[at : at + chunks]
        act_refs.append([own[0], None] + own[1:])
        at += chunks
    tok = grad_refs[0].shape[0]
    left_in = None
    if kind == "finish":
        left_in = refs[at]
        at += 1
    at += extra
    outs = refs[at : at + (1 if kind in ("left", "roots") else 3)]
    at += len(outs)
    acts_t, grads, gradient, current, factor, raised, later, pair, sems, out_sems = refs[at:]
    gather_block(
        ints, places, (owners, turns, tok, grad_refs, act_refs), acts_t, grads, sems
    )
    block_grad = wide_dot(acts_t[...], grads[...], 1, 0)
    if kind == "roots":
        block_grad = jnp.where(ints[3] != 0, block_grad, 0.0)
    block_grad = block_grad.astype(jnp.bfloat16)
    gradient[0] = block_grad
    if kind != "left":
        gradient[1] = block_grad.T
    squares = block_grad.astype(jnp.float32)
    square_sum = jnp.sum(squares * squares)
    params = (floats[0], ints[2], floats[1])
    work = (current, factor, raised, later)
    if kind == "left":
        inverse_root(0, gradient, outs[0], square_sum, params, *work)
        return
    if kind == "finish":
        inverse_root(1, gradient, pair.at[1], square_sum, params, *work)
        left_root = left_in[...]
    else:

        def one_side(side, carry):
            inverse_root(side, gradient, pair.at[side], square_sum, params, *work)
            if kind == "roots":
                pltpu.make_async_copy(
                    pair.at[side], outs[0].at[position, side], out_sems.at[side]
                ).start()
            return carry

        lax.fori_loop(0, 2, one_side, 0)
        left_root = pair[0]
    if kind == "roots":
        for side in range(2):
            pltpu.make_async_copy(
                pair.at[side], outs[0].at[position, side], out_sems.at[side]
            ).wait()
        return
    later[...] = wide_dot(left_root, gradient[0], 1, 0).astype(jnp.bfloat16)
    update = wide_dot(later[...], pair[1], 1, 0).astype(jnp.bfloat16)
    outs[0][...] = update[: BLK // 2]
    outs[1][...] = update[BLK // 2 :]
    wide = update.astype(jnp.float32)
    outs[2][0, 0] = jnp.sum(wide * wide)


def run_block(kind, job, meta, chunks, left_root=None, roots=None, position=0, count=1, after=()):
    ints, floats, places = meta
    grad_chunks, act_chunks = chunks
    owners = (len(grad_chunks) + 1) // 2
    turns = len(act_chunks)
    tokens = owners * grad_chunks[0].shape[0]
    smem = pl.BlockSpec(memory_space=pltpu.SMEM)
    vmem = pl.BlockSpec(memory_space=pltpu.VMEM)
    hbm = pl.BlockSpec(memory_space=HBM)
    operands = [ints, floats, places, *grad_chunks]
    for turn in act_chunks:
        operands += turn
    specs = [smem] * 3 + [hbm] * (len(operands) - 3)
    if left_root is not None:
        operands.append(left_root)
        specs.append(vmem)
    aliases = {}
    if roots is not None:
        aliases = {len(operands): 0}
        after = (roots, *after)
    operands += after
    specs += [hbm] * len(after)
    half = jnp.bfloat16
    piece = jax.ShapeDtypeStruct((BLK // 2, BLK), half)
    if kind == "left":
        out_shape, out_specs = jax.ShapeDtypeStruct((BLK, BLK), half), vmem
    elif kind == "roots":
        out_shape, out_specs = jax.ShapeDtypeStruct((count, 2, BLK, BLK), half), hbm
    else:
        out_shape = (piece, piece, jax.ShapeDtypeStruct((1, 1), jnp.float32))
        out_specs = (vmem, vmem, smem)
    matmuls = {"left": 6, "roots": 11, "finish": 8, "both": 13}[kind]
    return pl.pallas_call(
        functools.partial(block_kernel, kind, owners, turns, len(after), job, position),
        out_shape=out_shape,
        in_specs=specs,
        out_specs=out_specs,
        input_output_aliases=aliases,
        scratch_shapes=[
            pltpu.VMEM((BLK, tokens), half),
            pltpu.VMEM((tokens, BLK), half),
            pltpu.VMEM((2, BLK, BLK), half),
            pltpu.VMEM((BLK, BLK), half),
            pltpu.VMEM((BLK, BLK), half),
            pltpu.VMEM((2, BLK, BLK), half),
            pltpu.VMEM((BLK, BLK), half),
            pltpu.VMEM((2, BLK, BLK), half),
            pltpu.SemaphoreType.DMA((2 * (2 * owners - 1),)),
            pltpu.SemaphoreType.DMA((2,)),
        ],
        compiler_params=pltpu.CompilerParams(vmem_limit_bytes=VMEM_LIMIT),
        cost_estimate=pl.CostEstimate(
            flops=matmuls * 2 * BLK**3, bytes_accessed=6 * 2 * BLK**2, transcendentals=0
        ),
    )(*operands)


def place_kernel(first, count, late_count, extra, *refs):
    spots, rescale = refs[:2]
    pieces = refs[2 : 2 + count]
    canvas, held, in_sems, out_sems = refs[2 + count + extra :]
    near = late_count > 0
    rows = held.shape[1]
    loads = []
    stores = []
    for index in range(count):
        row = pl.multiple_of(spots[2 * (first + index)], rows)
        column = pl.multiple_of(spots[2 * (first + index) + 1], BLK)
        if not near:
            loads.append(pltpu.make_async_copy(pieces[index], held.at[index], in_sems.at[index]))
        stores.append(
            pltpu.make_async_copy(
                held.at[index],
                canvas.at[pl.ds(row, rows), pl.ds(column, BLK)],
                out_sems.at[index],
            )
        )
    if not near:
        for load in loads:
            load.start()
    for index in range(count):
        if not near:
            loads[index].wait()
        piece = pieces[index] if near else held.at[index]
        wide = piece[...].astype(jnp.float32) * rescale[0, 0]
        held[index] = wide.astype(jnp.bfloat16)
        stores[index].start()
    for store in stores:
        store.wait()


def place_pieces(canvas, shape, spots, first, rescale, pieces, late_count=0):
    count = len(pieces)
    smem = pl.BlockSpec(memory_space=pltpu.SMEM)
    hbm = pl.BlockSpec(memory_space=HBM)
    vmem = pl.BlockSpec(memory_space=pltpu.VMEM)
    old = [] if canvas is None else [canvas]
    return pl.pallas_call(
        functools.partial(place_kernel, first, count, late_count, len(old)),
        out_shape=jax.ShapeDtypeStruct(shape, jnp.bfloat16),
        in_specs=[smem, smem] + [vmem if late_count else hbm] * count + [hbm] * len(old),
        out_specs=hbm,
        input_output_aliases={2 + count: 0} if old else {},
        scratch_shapes=[
            pltpu.VMEM((count, *pieces[0].shape), jnp.bfloat16),
            pltpu.SemaphoreType.DMA((count,)),
            pltpu.SemaphoreType.DMA((count,)),
        ],
        compiler_params=pltpu.CompilerParams(vmem_limit_bytes=VMEM_LIMIT),
        cost_estimate=pl.CostEstimate(
            flops=count * BLK * BLK * 100, bytes_accessed=2 * count * BLK * BLK, transcendentals=0
        ),
        name="place",
    )(spots, rescale, *pieces, *old)


def ring_pairs(count):
    order = list(range(0, count, 2)) + list(range(1, count, 2))[::-1]
    ahead = [(order[i], order[(i + 1) % count]) for i in range(count)]
    back = [(b, a) for a, b in ahead]
    return order, ahead, back


def sum_steps(owners):
    bits = [1 << i for i in range((owners - 1).bit_length())]
    return dict(zip([0, 1, 3, 4, 2, *range(5, owners)], bits))


def shampoo_step(activations, out_grads, slot_table, exponent_index, damping_index):
    tok_count = activations.shape[0]
    row_blocks = activations.shape[1] // BLK
    half_width = out_grads.shape[1]
    col_blocks = half_width // BLK
    half_blocks = row_blocks * col_blocks
    owners = lax.axis_size("dp")
    halves = lax.axis_size("mp")
    me = lax.axis_index("dp")
    core = lax.axis_index("mp")
    slot_count = slot_table.shape[1]
    per_owner = slot_count // owners
    order, ahead, back = ring_pairs(owners)
    order_of = jnp.asarray(order, jnp.int32)
    place = jnp.asarray([order.index(i) for i in range(owners)], jnp.int32)[me]
    steps = jnp.arange(owners, dtype=jnp.int32)
    from_behind = order_of[(place - steps) % owners]
    from_ahead = order_of[(place + steps) % owners]
    places = jnp.concatenate([from_behind, from_ahead])

    table = slot_table[0, :half_blocks]
    exponents = exponent_index[0]
    dampings = damping_index[0]

    shared = min(owners, half_blocks)
    mine = jnp.minimum(me, shared - 1)
    block_range = jnp.arange(half_blocks, dtype=jnp.int32)
    slot_range = jnp.arange(slot_count, dtype=jnp.int32)
    spread = jnp.concatenate([mine[None], block_range[shared:]])
    spread_slots = jnp.sum(
        jnp.where(spread[:, None] == block_range[None, :], table[None, :], 0), axis=1
    )
    own_slots = me * per_owner + jnp.arange(per_owner, dtype=jnp.int32)
    matches = own_slots[:, None] == table[None, :]
    own_blocks = jnp.sum(jnp.where(matches, block_range[None, :], 0), axis=1)
    blocks = jnp.concatenate([spread, own_blocks])
    slots = jnp.concatenate([spread_slots, own_slots])
    filled = jnp.concatenate([jnp.ones_like(spread), jnp.any(matches, axis=1).astype(jnp.int32)])
    at_slot = slots[:, None] == slot_range[None, :]
    exp_picks = jnp.sum(jnp.where(at_slot, exponents[None, :], 0), axis=1)
    damp_picks = jnp.sum(jnp.where(at_slot, dampings[None, :], 0), axis=1)
    turn = (core - blocks // col_blocks) % halves
    ints = jnp.stack([turn, blocks % col_blocks, exp_picks, filled], axis=1).reshape(-1)
    floats = jnp.stack(
        [table_value(exp_picks, ROOT_ORDERS), table_value(damp_picks, DAMPINGS)], axis=1
    ).reshape(-1)
    late_count = 2
    rows = BLK // 2
    put_blocks = jnp.concatenate(
        [jnp.repeat(block_range[shared:], 2), jnp.stack([from_behind, from_ahead], 1).reshape(-1)]
    )
    put_blocks = jnp.minimum(put_blocks, half_blocks - 1)
    put_lower = jnp.tile(jnp.asarray([0, rows], jnp.int32), put_blocks.shape[0] // 2)
    spots = jnp.stack(
        [(put_blocks // col_blocks) * BLK + put_lower, (put_blocks % col_blocks) * BLK], axis=1
    ).reshape(-1)
    meta = (ints.astype(jnp.int32), floats, places, spots)

    part = activations.shape[1] // halves
    assert part == BLK
    act_part = lax.dynamic_slice(activations, (0, core * part), (tok_count, part)).T
    mp_shifts = [[(i, (i + s) % halves) for i in range(halves)] for s in range(1, halves)]
    half_tok = tok_count // 2
    half_row = part // 2

    grad_chunks = [out_grads]
    act_chunks = [[act_part]]
    for shift in mp_shifts:
        act_chunks.append([lax.ppermute(act_part, "mp", shift)])
    down, up = out_grads[:half_tok], out_grads[half_tok:]
    acts = (act_part[:half_row], act_part[half_row:])
    for step in range(1, owners):
        down = lax.ppermute(down, "dp", ahead)
        up = lax.ppermute(up, "dp", back)
        for act_step in (1, 2) if step == 1 else (step + 1,):
            if act_step < owners:
                acts = (lax.ppermute(acts[0], "dp", ahead), lax.ppermute(acts[1], "dp", back))
                act_chunks[0] += acts
                for turn, shift in enumerate(mp_shifts):
                    act_chunks[turn + 1] += [lax.ppermute(piece, "mp", shift) for piece in acts]
        if step == 2:
            down, up, acts, meta = lax.optimization_barrier((down, up, acts, meta))
        else:
            down, up, acts = lax.optimization_barrier((down, up, acts))
        grad_chunks += [down, up]
    chunks = (grad_chunks, act_chunks)

    spots = meta[3]
    meta = meta[:3]
    upper, lower, piece_sq = run_block("both", 0, meta, chunks)
    piece_sq = jnp.where(me < shared, piece_sq, 0.0)
    downs, ups = [upper], [lower]

    jobs = []
    rest = {}
    roots = [None]
    for job, block in enumerate(range(shared, half_blocks), 1):
        jobs.append(("left", lambda after, job=job, block=block: rest.__setitem__(
            block, run_block("left", job, meta, chunks, after=after)) or rest[block]))
        jobs.append(("finish", lambda after, job=job, block=block: rest.__setitem__(
            block, run_block("finish", job, meta, chunks, left_root=rest[block], after=after))
            or rest[block][0]))
    first = 1 + half_blocks - shared
    for position in range(per_owner):
        jobs.append(("roots", lambda after, position=position: roots.__setitem__(
            0, run_block("roots", first + position, meta, chunks, roots=roots[0],
                         position=position, count=per_owner, after=after)) or roots[0]))

    def exchange(value, axis, bit):
        pairs = [(i, i ^ bit) for i in range(lax.axis_size(axis))]
        return value + lax.ppermute(value, axis, pairs)

    half_sq = piece_sq
    sums = sum_steps(owners)
    if 0 in sums:
        half_sq = exchange(half_sq, "dp", sums[0])
        upper, lower, half_sq = lax.optimization_barrier((upper, lower, half_sq))
        downs, ups = [upper], [lower]
    for step in range(1, owners):
        after = (downs[-1], ups[-1]) if step > 1 else ()
        down = lax.ppermute(downs[-1], "dp", ahead)
        up = lax.ppermute(ups[-1], "dp", back)
        done = jobs.pop(0)[1](after) if jobs else half_sq
        if step in sums:
            half_sq, done = lax.optimization_barrier((half_sq, done))
            half_sq = exchange(half_sq, "dp", sums[step])
        if step < owners - 1:
            down, up, half_sq, _ = lax.optimization_barrier((down, up, half_sq, done))
        downs.append(down)
        ups.append(up)
    while jobs:
        jobs.pop(0)[1]((downs[-1], ups[-1]))
    for block in rest:
        half_sq = half_sq + rest[block][2]
    for bit in [1 << i for i in range((halves - 1).bit_length())]:
        half_sq = exchange(half_sq, "mp", bit)
    rescale = lax.rsqrt(half_sq / (row_blocks * BLK * half_width * halves) + 1.0)

    pieces = []
    for block in rest:
        pieces += rest[block][:2]
    for down, up in zip(downs, ups):
        pieces += [down, up]
    canvas = None
    limit = 20
    shape = (row_blocks * BLK, half_width)
    early = len(pieces) - late_count
    cuts = [*range(0, early, limit), early, len(pieces)]
    for low, high in zip(cuts[:-1], cuts[1:]):
        group = pieces[low:high]
        late = late_count if low == early else 0
        canvas = place_pieces(canvas, shape, spots, low, rescale, group, late)
    return canvas, roots[0][None]


def solution(mesh):
    placed = (
        P(("member", "dp"), None),
        P(("member", "dp"), "mp"),
        P(("member", "mp"), None),
        P(("member", "mp"), None),
        P(("member", "mp"), None),
    )
    return jax.shard_map(
        shampoo_step,
        mesh=mesh,
        in_specs=placed,
        out_specs=(P("member", "mp"), P(("member", "mp"), "dp", None, None, None)),
        check_vma=False,
    )
```
